128 devices in a mesh: gx: 8 (over z, x_lo), gy: 16 (over y, x_hi, core).
Axes of the slice: x: 4 (x_hi: 2, x_lo: 2; x = x_hi * 2 + x_lo), y: 4, z: 4, core: 2. Of those that a mesh axis runs over, the one named last changes fastest.
Arguments:
- probes: float32 [8, 128, 256, 512], P(None, 'gx', 'gy'), may hold values from -12.5 to 12.5, as said below
- disorder: float32 [128, 256, 512], P('gx', 'gy'), may hold values from -2 to 2
- spectrum_center: float32 [1], replicated, may hold values from -0.5 to 0.5
- half_width: float32 [1], replicated, may hold values from 9 to 11
Outputs:
- last_vector: float32 [8, 128, 256, 512], P(None, 'gx', 'gy')
- moments: float32 [8, 8], replicated
The draws below stay inside these ranges and needn't reach their ends.
Inputs may be any that keep to these rules, and one draw needn't show every extreme that they name: `probes`: real-valued probe entries.
All inputs are finite; a program needn't handle non-finite values.
Results may differ from the reference program's by a relative error of at most 0.0001.
Values sent between devices are 32-bit elements; how exact they have to be, the bound alone decides.
A program may use at most 128 MiB of HBM per device.

```python
import jax
import jax.numpy as jnp

PROBES = 8
NZ = 512
STEPS = 4
NX = 128
NY = 256


def draw_probes(key, part):
    first, second = jax.random.split(key, 2)
    shape = (PROBES, NX, NY, NZ)
    rough = jnp.exp(jax.random.uniform(second, shape, jnp.float32, -0.7, 0.7))
    rows_x = jnp.arange(NX, dtype=jnp.float32)[:, None]
    rows_y = jnp.arange(NY, dtype=jnp.float32)[None, :]
    frac = (rows_x * NY + rows_y) / (NX * NY - 1.0)
    base = jnp.clip(jax.random.normal(first, shape, jnp.float32), -4.0, 4.0)
    ramp = 0.5 + frac
    return (base * rough * ramp[None, :, :, None]).astype(jnp.float32)


def block_scale(rng, dims, shards, smallest, high):
    loudness, own = 1.0, jax.random.fold_in(rng, 6)
    for dim, parts in shards:
        heights = jnp.exp(jax.random.uniform(jax.random.fold_in(own, dim), (parts,), jnp.float32, smallest / len(shards), high / len(shards)))
        loudness = loudness * jnp.repeat(heights, dims[dim] // parts).reshape([-1 if axis == dim else 1 for axis in range(len(dims))])
    return loudness


def setup_inputs(seed: int = 0) -> dict:
    key_of = jax.random.split(jax.random.key(seed), 5)
    return {
        "probes": draw_probes(jax.random.fold_in(key_of[4], 71), 0),
        "disorder": jnp.clip(jax.random.uniform(key_of[1], (NX, NY, NZ), jnp.float32, -2.0, 2.0) * block_scale(key_of[1], (NX, NY, NZ), ((0, 8), (1, 16)), -0.4, 0.0), -2.0, 2.0),
        "spectrum_center": jnp.clip(jax.random.uniform(key_of[2], (1,), jnp.float32, -0.5, 0.5), -0.5, 0.5),
        "half_width": jnp.clip(jax.random.uniform(key_of[3], (1,), jnp.float32, 9.0, 11.0), 9.0, 11.0),
    }


def scaled_apply(ext, eps_part, center, width):
    core = ext[:, 1:-1, 1:-1]
    beside = ext[:, 2:, 1:-1] + ext[:, :-2, 1:-1] + ext[:, 1:-1, 2:] + ext[:, 1:-1, :-2]
    beside = beside + jnp.roll(core, 1, 3) + jnp.roll(core, -1, 3)
    return ((eps_part - center) * core - beside) / width


def padded(field):
    return jnp.pad(field, ((0, 0), (1, 1), (1, 1), (0, 0)), mode="wrap")


def inner_pair(t_low, t_high):
    square = jnp.sum(t_low * t_low, axis=(1, 2, 3))
    cross = jnp.sum(t_high * t_low, axis=(1, 2, 3))
    return jnp.stack([square, cross])


def reference(probes, disorder, spectrum_center, half_width):
    center = spectrum_center[0]
    width = half_width[0]
    energy = disorder[None]
    t_low = probes
    t_high = scaled_apply(padded(t_low), energy, center, width)
    collected = []
    for step in range(STEPS):
        collected.append(inner_pair(t_low, t_high))
        if step + 1 < STEPS:
            t_next = 2.0 * scaled_apply(padded(t_high), energy, center, width) - t_low
            t_low, t_high = t_high, t_next
    stacked = jnp.stack(collected)
    sites = jnp.float32(NX * NY * NZ)
    square = stacked[:, 0, :] / sites
    cross = stacked[:, 1, :] / sites
    even = 2.0 * square - square[0]
    odd = 2.0 * cross - cross[0]
    moments = jnp.stack([even, odd], axis=1).reshape(2 * STEPS, -1).T
    return t_high, moments
```

```python
import functools

import jax
import jax.numpy as jnp
from jax import lax
from jax.experimental import pallas as pl
from jax.experimental.pallas import tpu as pltpu
from jax.sharding import PartitionSpec as P

STEPS = 4
MESH = pl.DeviceIdType.MESH


def kernel(
    counts, center_ref, width_ref, probes_ref, disorder_ref, last_ref, sums_ref,
    field, last, energy, rim_y, edge_y, parts, load_sem, store_sem, send_sem, recv_sem
):
    probes, rows_x, rows_y, rows_z = probes_ref.shape
    n_gx, n_gy = counts
    gx, gy = lax.axis_index("gx"), lax.axis_index("gy")
    beside = (
        (lax.rem(gx + 1, n_gx), gy),
        (lax.rem(gx + n_gx - 1, n_gx), gy),
        (gx, lax.rem(gy + 1, n_gy)),
        (gx, lax.rem(gy + n_gy - 1, n_gy)),
    )

    def load(p):
        return pltpu.make_async_copy(
            probes_ref.at[p], field.at[0, p, pl.ds(1, rows_x)], load_sem.at[p]
        )

    def store(p):
        return pltpu.make_async_copy(last.at[p], last_ref.at[p], store_sem.at[p])

    def load_energy():
        return pltpu.make_async_copy(disorder_ref, energy, load_sem.at[probes])

    for p in range(probes):
        load(p).start()
    load_energy().start()

    barrier = pltpu.get_barrier_semaphore()
    for x, y in beside:
        pl.semaphore_signal(barrier, inc=1, device_id={"gx": x, "gy": y}, device_id_type=MESH)

    def sends(n, p):
        faces = (
            (field.at[n, p, rows_x], field.at[n, p, 0]),
            (field.at[n, p, 1], field.at[n, p, rows_x + 1]),
            (edge_y.at[n, p, 1], rim_y.at[n, p, 0]),
            (edge_y.at[n, p, 0], rim_y.at[n, p, 1]),
        )
        return [
            pltpu.make_async_remote_copy(
                src_ref=src,
                dst_ref=dst,
                send_sem=send_sem.at[n, p, f],
                recv_sem=recv_sem.at[n, p, f],
                device_id={"gx": beside[f][0], "gy": beside[f][1]},
                device_id_type=MESH,
            )
            for f, (src, dst) in enumerate(faces)
        ]

    for p in range(probes):
        load(p).wait()

        def pack(x, carry):
            edge_y[0, p, 0, pl.ds(x, 1), :] = field[0, p, x + 1, 0:1, :]
            edge_y[0, p, 1, pl.ds(x, 1), :] = field[0, p, x + 1, rows_y - 1 : rows_y, :]
            return carry

        lax.fori_loop(0, rows_x, pack, 0)
    load_energy().wait()
    energy[...] = energy[...] - center_ref[0]
    pl.semaphore_wait(barrier, 4)

    def first(p, carry):
        for copy in sends(0, p):
            copy.start()
        return carry

    lax.fori_loop(0, probes, first, 0)

    row = lax.broadcasted_iota(jnp.int32, (rows_y, rows_z), 0)
    scale = 1.0 / width_ref[0]

    def fold(square):
        total = square[0:8]
        for start in range(8, rows_y, 8):
            total = total + square[start : start + 8]
        out = total[:, 0:128]
        for start in range(128, rows_z, 128):
            out = out + total[:, start : start + 128]
        return out

    for n in range(STEPS):

        def probe(p, carry):
            for copy in sends(n, p):
                copy.wait_recv()

            def plane(x, acc):
                square, cross = acc
                core = field[n, p, x + 1]
                total = field[n, p, x] + field[n, p, x + 2]
                low = jnp.where(row == 0, rim_y[n, p, 0, pl.ds(x, 1), :], pltpu.roll(core, 1, 0))
                high = jnp.where(
                    row == rows_y - 1, rim_y[n, p, 1, pl.ds(x, 1), :], pltpu.roll(core, rows_y - 1, 0)
                )
                total = total + (low + high)
                total = total + (pltpu.roll(core, 1, 1) + pltpu.roll(core, rows_z - 1, 1))
                new = (energy[x] * core - total) * (scale if n == 0 else 2.0 * scale)
                if n > 0:
                    new = new - field[n - 1, p, x + 1]
                if n + 1 < STEPS:
                    field[n + 1, p, x + 1] = new
                    edge_y[n + 1, p, 0, pl.ds(x, 1), :] = new[0:1]
                    edge_y[n + 1, p, 1, pl.ds(x, 1), :] = new[rows_y - 1 : rows_y]
                else:
                    last[p, x] = new
                return square + fold(core * core), cross + fold(new * core)

            zero = jnp.zeros((8, 128), jnp.float32)
            square, cross = lax.fori_loop(0, rows_x, plane, (zero, zero))
            parts[2 * n, p] = square
            parts[2 * n + 1, p] = cross
            if n + 1 < STEPS:
                for copy in sends(n + 1, p):
                    copy.start()
            else:
                store(p).start()
            return carry

        lax.fori_loop(0, probes, probe, 0)

    lane = lax.broadcasted_iota(jnp.int32, (probes, 128), 1)
    sums = jnp.zeros((probes, 128), jnp.float32)
    for j in range(2 * STEPS):
        column = jnp.sum(jnp.sum(parts[j], axis=1), axis=1, keepdims=True)
        sums = jnp.where(lane == j, column, sums)
    sums_ref[...] = sums

    def drain(p, carry):
        for n in range(STEPS):
            for copy in sends(n, p):
                copy.wait_send()
        store(p).wait()
        return carry

    lax.fori_loop(0, probes, drain, 0)


def solution(mesh):
    counts = (mesh.shape["gx"], mesh.shape["gy"])

    def local(probes, disorder, spectrum_center, half_width):
        n_probes, rows_x, rows_y, rows_z = probes.shape
        smem = pl.BlockSpec(memory_space=pltpu.SMEM)
        hbm = pl.BlockSpec(memory_space=pl.ANY)
        last, sums = pl.pallas_call(
            functools.partial(kernel, counts),
            out_shape=(
                jax.ShapeDtypeStruct(probes.shape, jnp.float32),
                jax.ShapeDtypeStruct((n_probes, 128), jnp.float32),
            ),
            in_specs=[smem, smem, hbm, hbm],
            out_specs=(hbm, pl.BlockSpec(memory_space=pltpu.VMEM)),
            scratch_shapes=[
                pltpu.VMEM((STEPS, n_probes, rows_x + 2, rows_y, rows_z), jnp.float32),
                pltpu.VMEM((n_probes, rows_x, rows_y, rows_z), jnp.float32),
                pltpu.VMEM((rows_x, rows_y, rows_z), jnp.float32),
                pltpu.VMEM((STEPS, n_probes, 2, rows_x, rows_z), jnp.float32),
                pltpu.VMEM((STEPS, n_probes, 2, rows_x, rows_z), jnp.float32),
                pltpu.VMEM((2 * STEPS, n_probes, 8, 128), jnp.float32),
                pltpu.SemaphoreType.DMA((n_probes + 1,)),
                pltpu.SemaphoreType.DMA((n_probes,)),
                pltpu.SemaphoreType.DMA((STEPS, n_probes, 4)),
                pltpu.SemaphoreType.DMA((STEPS, n_probes, 4)),
            ],
            compiler_params=pltpu.CompilerParams(
                collective_id=0, has_side_effects=True, vmem_limit_bytes=48 * 1024 * 1024
            ),
        )(spectrum_center, half_width, probes, disorder)
        sums = lax.psum(sums[:, : 2 * STEPS], ("gx", "gy"))
        sites = jnp.float32(
            rows_x * counts[0] * rows_y * counts[1] * rows_z
        )
        mean = sums / sites
        base = jnp.tile(mean[:, :2], (1, STEPS))
        return last, 2.0 * mean - base

    return jax.shard_map(
        local,
        mesh=mesh,
        in_specs=(P(None, "gx", "gy", None), P("gx", "gy", None), P(), P()),
        out_specs=(P(None, "gx", "gy", None), P()),
        check_vma=False,
    )
```

```python
import functools

import jax
import jax.numpy as jnp
from jax import lax
from jax.experimental import pallas as pl
from jax.experimental.pallas import tpu as pltpu
from jax.sharding import PartitionSpec as P

STEPS = 4
MESH = pl.DeviceIdType.MESH


def kernel(
    counts, center_ref, width_ref, probes_ref, disorder_ref, last_ref, sums_ref,
    field, energy, rim_y, edge_y, parts, slots, load_sem, send_sem, recv_sem,
    slot_send, slot_recv
):
    probes, rows_x, rows_y, rows_z = probes_ref.shape
    n_gx, n_gy = counts
    gx, gy = lax.axis_index("gx"), lax.axis_index("gy")
    beside = (
        (lax.rem(gx + 1, n_gx), gy),
        (lax.rem(gx + n_gx - 1, n_gx), gy),
        (gx, lax.rem(gy + 1, n_gy)),
        (gx, lax.rem(gy + n_gy - 1, n_gy)),
    )

    def load(p):
        return pltpu.make_async_copy(
            probes_ref.at[p], field.at[0, p, pl.ds(1, rows_x)], load_sem.at[p]
        )

    def load_energy():
        return pltpu.make_async_copy(disorder_ref, energy, load_sem.at[probes])

    for p in range(probes):
        load(p).start()
    load_energy().start()

    x_lo, x_hi, core = lax.rem(gx, 2), lax.rem(gy // 2, 2), lax.rem(gy, 2)
    chip_x, chip_y, chip_z = 2 * x_hi + x_lo, gy // 4, gx // 2
    wide_y, wide_z = n_gy // 4, n_gx // 2

    def device(x, y, z, c):
        return (2 * z + lax.rem(x, 2), 4 * y + 2 * (x // 2) + c)

    groups = [[], [], []]
    for step in range(1, 8):
        x, c = lax.rem(chip_x + step // 2, 4), lax.rem(core + step, 2)
        groups[0].append((device(x, chip_y, chip_z, c), 2 * x + c))
    for step in range(1, wide_y):
        y = lax.rem(chip_y + step, wide_y)
        groups[1].append((device(chip_x, y, chip_z, core), y))
    for step in range(1, wide_z):
        z = lax.rem(chip_z + step, wide_z)
        groups[2].append((device(chip_x, chip_y, z, core), z))
    places = (2 * chip_x + core, chip_y, chip_z)
    sizes = (8, wide_y, wide_z)

    barrier = pltpu.get_barrier_semaphore()
    greeted = list(beside) + [peer for group in groups for peer, _ in group]
    for x, y in greeted:
        pl.semaphore_signal(barrier, inc=1, device_id={"gx": x, "gy": y}, device_id_type=MESH)

    def sends(n, p):
        faces = (
            (field.at[n, p, rows_x], field.at[n, p, 0]),
            (field.at[n, p, 1], field.at[n, p, rows_x + 1]),
            (edge_y.at[n, p, 1], rim_y.at[n, p, 0]),
            (edge_y.at[n, p, 0], rim_y.at[n, p, 1]),
        )
        return [
            pltpu.make_async_remote_copy(
                src_ref=src,
                dst_ref=dst,
                send_sem=send_sem.at[n, p, f],
                recv_sem=recv_sem.at[n, p, f],
                device_id={"gx": beside[f][0], "gy": beside[f][1]},
                device_id_type=MESH,
            )
            for f, (src, dst) in enumerate(faces)
        ]

    for p in range(probes):
        load(p).wait()

        def pack(x, carry):
            edge_y[0, p, 0, pl.ds(x, 1), :] = field[0, p, x + 1, 0:1, :]
            edge_y[0, p, 1, pl.ds(x, 1), :] = field[0, p, x + 1, rows_y - 1 : rows_y, :]
            return carry

        lax.fori_loop(0, rows_x, pack, 0)
    load_energy().wait()
    energy[...] = energy[...] - center_ref[0]
    pl.semaphore_wait(barrier, len(greeted))

    def first(p, carry):
        for copy in sends(0, p):
            copy.start()
        return carry

    lax.fori_loop(0, probes, first, 0)

    row = lax.broadcasted_iota(jnp.int32, (rows_y, rows_z), 0)
    scale = 1.0 / width_ref[0]

    def fold(square):
        total = square[0:8]
        for start in range(8, rows_y, 8):
            total = total + square[start : start + 8]
        out = total[:, 0:128]
        for start in range(128, rows_z, 128):
            out = out + total[:, start : start + 128]
        return out

    for n in range(STEPS):

        def probe(p, carry):
            for copy in sends(n, p):
                copy.wait_recv()

            def plane(x, acc):
                square, cross = acc
                core = field[n, p, x + 1]
                total = field[n, p, x] + field[n, p, x + 2]
                low = jnp.where(row == 0, rim_y[n, p, 0, pl.ds(x, 1), :], pltpu.roll(core, 1, 0))
                high = jnp.where(
                    row == rows_y - 1, rim_y[n, p, 1, pl.ds(x, 1), :], pltpu.roll(core, rows_y - 1, 0)
                )
                total = total + (low + high)
                total = total + (pltpu.roll(core, 1, 1) + pltpu.roll(core, rows_z - 1, 1))
                new = (energy[x] * core - total) * (scale if n == 0 else 2.0 * scale)
                if n > 0:
                    new = new - field[n - 1, p, x + 1]
                if n + 1 < STEPS:
                    field[n + 1, p, x + 1] = new
                    edge_y[n + 1, p, 0, pl.ds(x, 1), :] = new[0:1]
                    edge_y[n + 1, p, 1, pl.ds(x, 1), :] = new[rows_y - 1 : rows_y]
                else:
                    last_ref[p, x] = new
                return square + fold(core * core), cross + fold(new * core)

            zero = jnp.zeros((8, 128), jnp.float32)
            square, cross = lax.fori_loop(0, rows_x, plane, (zero, zero))
            parts[2 * n, p] = square
            parts[2 * n + 1, p] = cross
            if n + 1 < STEPS:
                for copy in sends(n + 1, p):
                    copy.start()
            return carry

        lax.fori_loop(0, probes, probe, 0)

    lane = lax.broadcasted_iota(jnp.int32, (probes, 128), 1)
    sums = jnp.zeros((probes, 128), jnp.float32)
    for j in range(2 * STEPS):
        column = jnp.sum(jnp.sum(parts[j], axis=1), axis=1, keepdims=True)
        sums = jnp.where(lane == j, column, sums)

    for g, group in enumerate(groups):
        place = places[g]
        slots[g, place] = sums
        copies = [
            pltpu.make_async_remote_copy(
                src_ref=slots.at[g, place],
                dst_ref=slots.at[g, place],
                send_sem=slot_send.at[g, i],
                recv_sem=slot_recv.at[g, place],
                device_id={"gx": peer[0], "gy": peer[1]},
                device_id_type=MESH,
            )
            for i, (peer, _) in enumerate(group)
        ]
        for copy in copies:
            copy.start()
        for peer, slot in group:
            pltpu.make_async_remote_copy(
                src_ref=slots.at[g, slot],
                dst_ref=slots.at[g, slot],
                send_sem=slot_send.at[g, 0],
                recv_sem=slot_recv.at[g, slot],
                device_id={"gx": peer[0], "gy": peer[1]},
                device_id_type=MESH,
            ).wait_recv()
        sums = slots[g, 0]
        for i in range(1, sizes[g]):
            sums = sums + slots[g, i]
        for copy in copies:
            copy.wait_send()
    sums_ref[...] = sums

    def drain(p, carry):
        for n in range(STEPS):
            for copy in sends(n, p):
                copy.wait_send()
        return carry

    lax.fori_loop(0, probes, drain, 0)


def finish(sites, last_ref, sums_ref, out_ref, moments_ref, sem):
    probes = last_ref.shape[0]
    copies = [
        pltpu.make_async_copy(last_ref.at[p], out_ref.at[p], sem.at[p]) for p in range(probes)
    ]
    for copy in copies:
        copy.start()
    mean = sums_ref[...] * (1.0 / sites)
    lane = lax.broadcasted_iota(jnp.int32, mean.shape, 1)
    base = jnp.where(lax.rem(lane, 2) == 0, mean[:, 0:1], mean[:, 1:2])
    moments_ref[...] = (2.0 * mean - base)[:, : 2 * STEPS]
    for copy in copies:
        copy.wait()


def solution(mesh):
    counts = (mesh.shape["gx"], mesh.shape["gy"])

    def local(probes, disorder, spectrum_center, half_width):
        n_probes, rows_x, rows_y, rows_z = probes.shape
        smem = pl.BlockSpec(memory_space=pltpu.SMEM)
        vmem = pl.BlockSpec(memory_space=pltpu.VMEM)
        hbm = pl.BlockSpec(memory_space=pltpu.HBM)
        last, sums = pl.pallas_call(
            functools.partial(kernel, counts),
            out_shape=(
                jax.ShapeDtypeStruct(probes.shape, jnp.float32),
                jax.ShapeDtypeStruct((n_probes, 128), jnp.float32),
            ),
            in_specs=[smem, smem, hbm, hbm],
            out_specs=(vmem, vmem),
            scratch_shapes=[
                pltpu.VMEM((STEPS, n_probes, rows_x + 2, rows_y, rows_z), jnp.float32),
                pltpu.VMEM((rows_x, rows_y, rows_z), jnp.float32),
                pltpu.VMEM((STEPS, n_probes, 2, rows_x, rows_z), jnp.float32),
                pltpu.VMEM((STEPS, n_probes, 2, rows_x, rows_z), jnp.float32),
                pltpu.VMEM((2 * STEPS, n_probes, 8, 128), jnp.float32),
                pltpu.VMEM((3, 8, n_probes, 128), jnp.float32),
                pltpu.SemaphoreType.DMA((n_probes + 1,)),
                pltpu.SemaphoreType.DMA((STEPS, n_probes, 4)),
                pltpu.SemaphoreType.DMA((STEPS, n_probes, 4)),
                pltpu.SemaphoreType.DMA((3, 8)),
                pltpu.SemaphoreType.DMA((3, 8)),
            ],
            compiler_params=pltpu.CompilerParams(
                collective_id=0, has_side_effects=True, vmem_limit_bytes=48 * 1024 * 1024
            ),
        )(spectrum_center, half_width, probes, disorder)
        sites = rows_x * counts[0] * rows_y * counts[1] * rows_z
        return pl.pallas_call(
            functools.partial(finish, sites),
            out_shape=(
                jax.ShapeDtypeStruct(probes.shape, jnp.float32),
                jax.ShapeDtypeStruct((n_probes, 2 * STEPS), jnp.float32),
            ),
            in_specs=[vmem, vmem],
            out_specs=(hbm, vmem),
            scratch_shapes=[pltpu.SemaphoreType.DMA((n_probes,))],
            compiler_params=pltpu.CompilerParams(vmem_limit_bytes=8 * 1024 * 1024),
        )(last, sums)

    return jax.shard_map(
        local,
        mesh=mesh,
        in_specs=(P(None, "gx", "gy", None), P("gx", "gy", None), P(), P()),
        out_specs=(P(None, "gx", "gy", None), P()),
        check_vma=False,
    )
```

```python
import functools

import jax
import jax.numpy as jnp
from jax import lax
from jax.experimental import pallas as pl
from jax.experimental.pallas import tpu as pltpu
from jax.sharding import PartitionSpec as P

STEPS = 4
BATCH = 1
MESH = pl.DeviceIdType.MESH
LEAD = 4
UNROLL = 8
LATER = (2, 2, 8)
FINISH = (2, 2, 8)
VMEM_LIMIT = 48 * 1024 * 1024


def kernel(
    counts, center_ref, width_ref, probes_ref, disorder_ref, last_ref, sums_ref,
    field, energy, rim_y, edge_y, parts, slots, load_sem, send_sem, recv_sem,
    slot_send, slot_recv
):
    probes, rows_x, rows_y, rows_z = probes_ref.shape
    batches = probes // BATCH
    n_gx, n_gy = counts
    gx, gy = lax.axis_index("gx"), lax.axis_index("gy")
    beside = (
        (lax.rem(gx + 1, n_gx), gy),
        (lax.rem(gx + n_gx - 1, n_gx), gy),
        (gx, lax.rem(gy + 1, n_gy)),
        (gx, lax.rem(gy + n_gy - 1, n_gy)),
    )
    x_lo, x_hi, core = lax.rem(gx, 2), lax.rem(gy // 2, 2), lax.rem(gy, 2)
    chip_x, chip_y, chip_z = 2 * x_hi + x_lo, gy // 4, gx // 2
    wide_y, wide_z = n_gy // 4, n_gx // 2

    def device(x, y, z, c):
        return (2 * z + lax.rem(x, 2), 4 * y + 2 * (x // 2) + c)

    group_x, group_y, group_z = [], [], []
    for step in range(1, 8):
        x, c = lax.rem(chip_x + step // 2, 4), lax.rem(core + step, 2)
        group_x.append(device(x, chip_y, chip_z, c))
    for step in range(1, wide_y):
        group_y.append(device(chip_x, lax.rem(chip_y + step, wide_y), chip_z, core))
    for step in range(1, wide_z):
        group_z.append(device(chip_x, chip_y, lax.rem(chip_z + step, wide_z), core))
    groups = ((group_z, chip_z), (group_y, chip_y), (group_x, 2 * chip_x + core))

    barrier = pltpu.get_barrier_semaphore()
    greeted = list(beside) + group_z + group_y + group_x
    for x, y in greeted:
        pl.semaphore_signal(barrier, inc=1, device_id={"gx": x, "gy": y}, device_id_type=MESH)

    def load(p):
        return pltpu.make_async_copy(
            probes_ref.at[p], field.at[0, p, pl.ds(1, rows_x)], load_sem.at[p]
        )

    def load_energy():
        return pltpu.make_async_copy(disorder_ref, energy, load_sem.at[probes])

    for p in range(probes):
        load(p).start()
    load_energy().start()

    def faces(n, b):
        group = pl.ds(b * BATCH, BATCH)
        return (
            (field.at[n, group, rows_x], field.at[n, group, 0]),
            (field.at[n, group, 1], field.at[n, group, rows_x + 1]),
            (edge_y.at[n, 1, group], rim_y.at[n, 0, group]),
            (edge_y.at[n, 0, group], rim_y.at[n, 1, group]),
        )

    def send(n, b, which, sem):
        for f in which:
            src, dst = faces(n, b)[f]
            pltpu.make_async_remote_copy(
                src_ref=src,
                dst_ref=dst,
                send_sem=send_sem.at[sem, b],
                recv_sem=recv_sem.at[sem, b],
                device_id={"gx": beside[f][0], "gy": beside[f][1]},
                device_id_type=MESH,
            ).start()

    def settled(b, count, sem):
        whole = field.at[0, 0, pl.ds(0, count * BATCH)]
        return pltpu.make_async_remote_copy(
            src_ref=whole,
            dst_ref=whole,
            send_sem=send_sem.at[sem, b],
            recv_sem=recv_sem.at[sem, b],
            device_id={"gx": beside[0][0], "gy": beside[0][1]},
            device_id_type=MESH,
        )

    for p in range(probes):
        load(p).wait()

        def pack(x, carry):
            edge_y[0, 0, p, pl.ds(x, 1), :] = field[0, p, x + 1, 0:1, :]
            edge_y[0, 1, p, pl.ds(x, 1), :] = field[0, p, x + 1, rows_y - 1 : rows_y, :]
            return carry

        lax.fori_loop(0, rows_x, pack, 0)
    load_energy().wait()
    energy[...] = energy[...] - center_ref[0]
    pl.semaphore_wait(barrier, len(greeted))

    for b in range(batches):
        send(0, b, (0, 1, 2, 3), 0)

    row = lax.broadcasted_iota(jnp.int32, (rows_y, rows_z), 0)
    scale = 1.0 / width_ref[0]
    zero = jnp.zeros((8, 128), jnp.float32)

    def fold(product):
        total = product[0:8]
        for start in range(8, rows_y, 8):
            total = total + product[start : start + 8]
        out = total[:, 0:128]
        for start in range(128, rows_z, 128):
            out = out + total[:, start : start + 128]
        return out

    def low_side(n, p, x, middle):
        y = jnp.where(row == 0, rim_y[n, 0, p, pl.ds(x, 1), :], pltpu.roll(middle, 1, 0))
        return field[n, p, x] + y + pltpu.roll(middle, 1, 1)

    def high_side(n, p, x, middle):
        y = jnp.where(
            row == rows_y - 1, rim_y[n, 1, p, pl.ds(x, 1), :], pltpu.roll(middle, rows_y - 1, 0)
        )
        return field[n, p, x + 2] + y + pltpu.roll(middle, rows_z - 1, 1)

    def advance(n, p):
        def plane(x, acc):
            square, cross = acc
            middle = field[n, p, x + 1]
            total = low_side(n, p, x, middle) + high_side(n, p, x, middle)
            new = (energy[x] * middle - total) * (scale if n == 0 else 2.0 * scale)
            if n > 0:
                new = new - field[n - 1, p, x + 1]
            field[n + 1, p, x + 1] = new
            edge_y[n + 1, 0, p, pl.ds(x, 1), :] = new[0:1]
            edge_y[n + 1, 1, p, pl.ds(x, 1), :] = new[rows_y - 1 : rows_y]
            return square + fold(middle * middle), cross + fold(new * middle)

        parts[2 * n, p], parts[2 * n + 1, p] = lax.fori_loop(0, rows_x, plane, (zero, zero), unroll=UNROLL)

    final = STEPS - 1

    def last_low(p):
        def plane(x, acc):
            square, cross = acc
            middle = field[final, p, x + 1]
            low = (2.0 * scale) * low_side(final, p, x, middle)
            new = (2.0 * scale) * energy[x] * middle - low - field[final - 1, p, x + 1]
            last_ref[p, x] = new
            return square + fold(middle * middle), cross + fold((new - low) * middle)

        parts[2 * final, p], parts[2 * final + 1, p] = lax.fori_loop(0, rows_x, plane, (zero, zero), unroll=UNROLL)

    def last_high(p):
        def plane(x, carry):
            middle = field[final, p, x + 1]
            last_ref[p, x] = last_ref[p, x] - (2.0 * scale) * high_side(final, p, x, middle)
            return carry

        lax.fori_loop(0, rows_x, plane, 0, unroll=UNROLL)

    for n in range(final):

        def batch(b, carry):
            settled(b, 4, n % 2).wait_recv()

            def one(q, carry):
                advance(n, b * BATCH + q)
                return carry

            lax.fori_loop(0, BATCH, one, 0)
            if n > 0:
                settled(b, 4, (n + 1) % 2).wait_send()
            send(n + 1, b, (0, 1, 2, 3) if n + 1 < final else (0, 2), (n + 1) % 2)
            return carry

        lax.fori_loop(0, batches, batch, 0)

    sent, done = [0], [0]

    def send_more(count):
        for _ in range(count):
            if sent[0] < batches:
                send(final, sent[0], (1, 3), 2)
                sent[0] += 1

    def finish_more(count):
        for _ in range(count):
            if done[0] < sent[0]:
                settled(done[0], 2, 2).wait_recv()

                def one(q, carry, b=done[0]):
                    last_high(b * BATCH + q)
                    return carry

                lax.fori_loop(0, BATCH, one, 0)
                done[0] += 1

    for b in range(batches):
        settled(b, 2, final % 2).wait_recv()

        def one(q, carry, b=b):
            last_low(b * BATCH + q)
            return carry

        lax.fori_loop(0, BATCH, one, 0)
        if b >= LEAD:
            send_more(1)

    lane = lax.broadcasted_iota(jnp.int32, (probes, 128), 1)
    sums = jnp.zeros((probes, 128), jnp.float32)
    for j in range(2 * STEPS):
        column = jnp.sum(jnp.sum(parts[j], axis=1), axis=1, keepdims=True)
        sums = jnp.where(lane == j, column, sums)

    for g, (group, place) in enumerate(groups):
        slots[g, place] = sums
        for x, y in group:
            pltpu.make_async_remote_copy(
                src_ref=slots.at[g, place],
                dst_ref=slots.at[g, place],
                send_sem=slot_send.at[g],
                recv_sem=slot_recv.at[g],
                device_id={"gx": x, "gy": y},
                device_id_type=MESH,
            ).start()
        send_more(LATER[g])
        finish_more(FINISH[g])
        whole = slots.at[g, pl.ds(0, len(group))]
        arrived = pltpu.make_async_remote_copy(
            src_ref=whole,
            dst_ref=whole,
            send_sem=slot_send.at[g],
            recv_sem=slot_recv.at[g],
            device_id={"gx": group[0][0], "gy": group[0][1]},
            device_id_type=MESH,
        )
        arrived.wait_recv()
        sums = slots[g, 0]
        for i in range(1, len(group) + 1):
            sums = sums + slots[g, i]
        arrived.wait_send()
    sums_ref[...] = sums
    finish_more(batches)

    for b in range(batches):
        settled(b, 4, (final - 1) % 2).wait_send()
        settled(b, 2, final % 2).wait_send()
        settled(b, 2, 2).wait_send()


def finish(sites, last_ref, sums_ref, out_ref, moments_ref, sem):
    probes = last_ref.shape[0]
    copies = [
        pltpu.make_async_copy(last_ref.at[p], out_ref.at[p], sem.at[p]) for p in range(probes)
    ]
    for copy in copies:
        copy.start()
    mean = sums_ref[...] * (1.0 / sites)
    lane = lax.broadcasted_iota(jnp.int32, mean.shape, 1)
    base = jnp.where(lax.rem(lane, 2) == 0, mean[:, 0:1], mean[:, 1:2])
    moments_ref[...] = (2.0 * mean - base)[:, : 2 * STEPS]
    for copy in copies:
        copy.wait()


def solution(mesh):
    counts = (mesh.shape["gx"], mesh.shape["gy"])

    def local(probes, disorder, spectrum_center, half_width):
        n_probes, rows_x, rows_y, rows_z = probes.shape
        disorder = pltpu.with_memory_space_constraint(disorder, pltpu.HBM)
        smem = pl.BlockSpec(memory_space=pltpu.SMEM)
        vmem = pl.BlockSpec(memory_space=pltpu.VMEM)
        hbm = pl.BlockSpec(memory_space=pltpu.HBM)
        last, sums = pl.pallas_call(
            functools.partial(kernel, counts),
            out_shape=(
                jax.ShapeDtypeStruct(probes.shape, jnp.float32),
                jax.ShapeDtypeStruct((n_probes, 128), jnp.float32),
            ),
            in_specs=[smem, smem, hbm, hbm],
            out_specs=(vmem, vmem),
            scratch_shapes=[
                pltpu.VMEM((STEPS, n_probes, rows_x + 2, rows_y, rows_z), jnp.float32),
                pltpu.VMEM((rows_x, rows_y, rows_z), jnp.float32),
                pltpu.VMEM((STEPS, 2, n_probes, rows_x, rows_z), jnp.float32),
                pltpu.VMEM((STEPS, 2, n_probes, rows_x, rows_z), jnp.float32),
                pltpu.VMEM((2 * STEPS, n_probes, 8, 128), jnp.float32),
                pltpu.VMEM((3, 8, n_probes, 128), jnp.float32),
                pltpu.SemaphoreType.DMA((n_probes + 1,)),
                pltpu.SemaphoreType.DMA((3, n_probes // BATCH)),
                pltpu.SemaphoreType.DMA((3, n_probes // BATCH)),
                pltpu.SemaphoreType.DMA((3,)),
                pltpu.SemaphoreType.DMA((3,)),
            ],
            compiler_params=pltpu.CompilerParams(
                collective_id=0, has_side_effects=True, vmem_limit_bytes=VMEM_LIMIT
            ),
        )(spectrum_center, half_width, probes, disorder)
        sites = rows_x * counts[0] * rows_y * counts[1] * rows_z
        return pl.pallas_call(
            functools.partial(finish, sites),
            out_shape=(
                jax.ShapeDtypeStruct(probes.shape, jnp.float32),
                jax.ShapeDtypeStruct((n_probes, 2 * STEPS), jnp.float32),
            ),
            in_specs=[vmem, vmem],
            out_specs=(hbm, vmem),
            scratch_shapes=[pltpu.SemaphoreType.DMA((n_probes,))],
            compiler_params=pltpu.CompilerParams(vmem_limit_bytes=8 * 1024 * 1024),
        )(last, sums)

    return jax.shard_map(
        local,
        mesh=mesh,
        in_specs=(P(None, "gx", "gy", None), P("gx", "gy", None), P(), P()),
        out_specs=(P(None, "gx", "gy", None), P()),
        check_vma=False,
    )
```

```python
import functools

import jax
import jax.numpy as jnp
from jax import lax
from jax.experimental import pallas as pl
from jax.experimental.pallas import tpu as pltpu
from jax.sharding import PartitionSpec as P

STEPS = 4
BATCH = 1
MESH = pl.DeviceIdType.MESH
LEAD = 4
ORDER = (0, 1, 2, 3)
UNROLL = 8
LATER = (2, 2, 8)
FINISH = (2, 2, 8)
VMEM_LIMIT = 48 * 1024 * 1024


def kernel(
    counts, center_ref, width_ref, probes_ref, disorder_ref, last_ref, sums_ref,
    field, energy, rim_y, edge_y, parts, slots, load_sem, send_sem, recv_sem,
    slot_send, slot_recv, ready
):
    probes, rows_x, rows_y, rows_z = probes_ref.shape
    batches = probes // BATCH
    n_gx, n_gy = counts
    gx, gy = lax.axis_index("gx"), lax.axis_index("gy")
    beside = (
        (lax.rem(gx + 1, n_gx), gy),
        (lax.rem(gx + n_gx - 1, n_gx), gy),
        (gx, lax.rem(gy + 1, n_gy)),
        (gx, lax.rem(gy + n_gy - 1, n_gy)),
    )
    x_lo, x_hi, core = lax.rem(gx, 2), lax.rem(gy // 2, 2), lax.rem(gy, 2)
    chip_x, chip_y, chip_z = 2 * x_hi + x_lo, gy // 4, gx // 2
    wide_y, wide_z = n_gy // 4, n_gx // 2

    def device(x, y, z, c):
        return (2 * z + lax.rem(x, 2), 4 * y + 2 * (x // 2) + c)

    def group(pairs):
        return [device(lax.rem(chip_x + x, 4), lax.rem(chip_y + y, wide_y), lax.rem(chip_z + z, wide_z),
                       lax.rem(core + c, 2)) for x, y, z, c in pairs]

    group_x = group([(x, 0, 0, c) for x in range(4) for c in range(2) if x or c])
    group_y = group([(0, y, 0, 0) for y in range(1, wide_y)])
    group_z = group([(0, 0, z, 0) for z in range(1, wide_z)])
    groups = ((group_z, chip_z), (group_y, chip_y), (group_x, 2 * chip_x + core))

    partner = (gx + 1 - 2 * x_lo, gy)
    across = (lax.rem(gx + 2 * x_lo + n_gx - 1, n_gx), gy)
    pairs = list(beside[2:]) + group_z + group_y + group([(2, 0, 0, 0), (0, 0, 0, 1), (2, 0, 0, 1)])
    barrier = pltpu.get_barrier_semaphore()

    def tell(semaphore, peer):
        pl.semaphore_signal(
            semaphore, inc=1, device_id={"gx": peer[0], "gy": peer[1]}, device_id_type=MESH
        )

    @pl.when(x_lo == 1)
    def _():
        tell(barrier, partner)

    for x, y in pairs:
        tell(barrier, (x + 1 - lax.rem(x, 2), y))

    def load(p):
        return pltpu.make_async_copy(
            probes_ref.at[p], field.at[0, p, pl.ds(1, rows_x)], load_sem.at[p]
        )

    def load_energy():
        return pltpu.make_async_copy(disorder_ref, energy, load_sem.at[probes])

    for p in range(probes):
        load(p).start()
    load_energy().start()

    def faces(n, b):
        group = pl.ds(b * BATCH, BATCH)
        return (
            (field.at[n, group, rows_x], field.at[n, group, 0]),
            (field.at[n, group, 1], field.at[n, group, rows_x + 1]),
            (edge_y.at[n, 1, group], rim_y.at[n, 0, group]),
            (edge_y.at[n, 0, group], rim_y.at[n, 1, group]),
        )

    def start(src, dst, peer, sem, b):
        pltpu.make_async_remote_copy(
            src_ref=src,
            dst_ref=dst,
            send_sem=send_sem.at[sem, b],
            recv_sem=recv_sem.at[sem, b],
            device_id={"gx": peer[0], "gy": peer[1]},
            device_id_type=MESH,
        ).start()

    def send(n, b, which, sem):
        for f in which:
            src, dst = faces(n, b)[f]
            start(src, dst, beside[f], sem, b)

    def settled(b, count, sem):
        whole = field.at[0, 0, pl.ds(0, count * BATCH)]
        return pltpu.make_async_remote_copy(
            src_ref=whole,
            dst_ref=whole,
            send_sem=send_sem.at[sem, b],
            recv_sem=recv_sem.at[sem, b],
            device_id={"gx": beside[0][0], "gy": beside[0][1]},
            device_id_type=MESH,
        )

    @pl.when(x_lo == 0)
    def _():
        pl.semaphore_wait(barrier, 1)
        tell(ready.at[0], partner)

    @pl.when(x_lo == 1)
    def _():
        pl.semaphore_wait(ready.at[0], 1)

    for b in range(batches):
        for p in range(b * BATCH, b * BATCH + BATCH):
            load(p).wait()
        which = pl.ds(b * BATCH, BATCH)
        start(
            field.at[0, which, rows_x - (rows_x - 1) * x_lo],
            field.at[0, which, (rows_x + 1) * x_lo],
            partner, 0, b,
        )

    def pack(p, carry):
        for x in range(rows_x):
            edge_y[0, 0, p, x : x + 1, :] = field[0, p, x + 1, 0:1, :]
            edge_y[0, 1, p, x : x + 1, :] = field[0, p, x + 1, rows_y - 1 : rows_y, :]
        return carry

    lax.fori_loop(0, probes, pack, 0)

    @pl.when(x_lo == 1)
    def _():
        pl.semaphore_wait(barrier, 2 * len(pairs))
        tell(ready.at[1], partner)

    @pl.when(x_lo == 0)
    def _():
        pl.semaphore_wait(ready.at[1], 1)

    for b in range(batches):
        which = pl.ds(b * BATCH, BATCH)
        start(
            field.at[0, which, 1 + (rows_x - 1) * x_lo],
            field.at[0, which, (rows_x + 1) * (1 - x_lo)],
            across, 0, b,
        )
        send(0, b, (2, 3), 0)
    load_energy().wait()
    energy[...] = energy[...] - center_ref[0]

    row = lax.broadcasted_iota(jnp.int32, (rows_y, rows_z), 0)
    scale = 1.0 / width_ref[0]
    zero = jnp.zeros((8, 128), jnp.float32)

    def fold(product):
        total = product[0:8]
        for start in range(8, rows_y, 8):
            total = total + product[start : start + 8]
        out = total[:, 0:128]
        for start in range(128, rows_z, 128):
            out = out + total[:, start : start + 128]
        return out

    def low_side(n, p, x, middle):
        y = jnp.where(row == 0, rim_y[n, 0, p, pl.ds(x, 1), :], pltpu.roll(middle, 1, 0))
        return field[n, p, x] + y + pltpu.roll(middle, 1, 1)

    def high_side(n, p, x, middle):
        y = jnp.where(
            row == rows_y - 1, rim_y[n, 1, p, pl.ds(x, 1), :], pltpu.roll(middle, rows_y - 1, 0)
        )
        return field[n, p, x + 2] + y + pltpu.roll(middle, rows_z - 1, 1)

    def advance(n, p):
        def plane(x, acc):
            square, cross = acc
            middle = field[n, p, x + 1]
            total = low_side(n, p, x, middle) + high_side(n, p, x, middle)
            new = (energy[x] * middle - total) * (scale if n == 0 else 2.0 * scale)
            if n > 0:
                new = new - field[n - 1, p, x + 1]
            field[n + 1, p, x + 1] = new
            edge_y[n + 1, 0, p, pl.ds(x, 1), :] = new[0:1]
            edge_y[n + 1, 1, p, pl.ds(x, 1), :] = new[rows_y - 1 : rows_y]
            return square + fold(middle * middle), cross + fold(new * middle)

        parts[2 * n, p], parts[2 * n + 1, p] = lax.fori_loop(0, rows_x, plane, (zero, zero), unroll=UNROLL)

    final = STEPS - 1

    def last_low(p):
        def plane(x, acc):
            square, cross = acc
            middle = field[final, p, x + 1]
            low = (2.0 * scale) * low_side(final, p, x, middle)
            new = (2.0 * scale) * energy[x] * middle - low - field[final - 1, p, x + 1]
            last_ref[p, x] = new
            return square + fold(middle * middle), cross + fold((new - low) * middle)

        parts[2 * final, p], parts[2 * final + 1, p] = lax.fori_loop(0, rows_x, plane, (zero, zero), unroll=UNROLL)

    def last_high(p):
        def plane(x, carry):
            middle = field[final, p, x + 1]
            last_ref[p, x] = last_ref[p, x] - (2.0 * scale) * high_side(final, p, x, middle)
            return carry

        lax.fori_loop(0, rows_x, plane, 0, unroll=UNROLL)

    for n in range(final):

        def batch(b, carry):
            settled(b, 4, n % 2).wait_recv()

            def one(q, carry):
                advance(n, b * BATCH + q)
                return carry

            lax.fori_loop(0, BATCH, one, 0)
            if n > 0:
                settled(b, 4, (n + 1) % 2).wait_send()
            send(n + 1, b, ORDER if n + 1 < final else (0, 2), (n + 1) % 2)
            return carry

        lax.fori_loop(0, batches, batch, 0)

    sent, done = [0], [0]

    def send_more(count):
        for _ in range(count):
            if sent[0] < batches:
                send(final, sent[0], (1, 3), 2)
                sent[0] += 1

    def finish_more(count):
        for _ in range(count):
            if done[0] < sent[0]:
                settled(done[0], 2, 2).wait_recv()

                def one(q, carry, b=done[0]):
                    last_high(b * BATCH + q)
                    return carry

                lax.fori_loop(0, BATCH, one, 0)
                done[0] += 1

    lane = lax.broadcasted_iota(jnp.int32, (probes, 128), 1)

    def column_sums(sums, columns):
        for j in columns:
            column = jnp.sum(jnp.sum(parts[j], axis=1), axis=1, keepdims=True)
            sums = jnp.where(lane == j, column, sums)
        return sums

    sums = column_sums(jnp.zeros((probes, 128), jnp.float32), range(2 * final))

    for b in range(batches):
        settled(b, 2, final % 2).wait_recv()

        def one(q, carry, b=b):
            last_low(b * BATCH + q)
            return carry

        lax.fori_loop(0, BATCH, one, 0)
        if b >= LEAD:
            send_more(1)

    sums = column_sums(sums, range(2 * final, 2 * STEPS))

    for g, (peers, place) in enumerate(groups):
        slots[g, place] = sums
        for x, y in peers:
            pltpu.make_async_remote_copy(
                src_ref=slots.at[g, place],
                dst_ref=slots.at[g, place],
                send_sem=slot_send.at[g],
                recv_sem=slot_recv.at[g],
                device_id={"gx": x, "gy": y},
                device_id_type=MESH,
            ).start()
        send_more(LATER[g])
        finish_more(FINISH[g])
        whole = slots.at[g, pl.ds(0, len(peers))]
        arrived = pltpu.make_async_remote_copy(
            src_ref=whole,
            dst_ref=whole,
            send_sem=slot_send.at[g],
            recv_sem=slot_recv.at[g],
            device_id={"gx": peers[0][0], "gy": peers[0][1]},
            device_id_type=MESH,
        )
        arrived.wait_recv()
        sums = slots[g, 0]
        for i in range(1, len(peers) + 1):
            sums = sums + slots[g, i]
        arrived.wait_send()
    sums_ref[...] = sums
    finish_more(batches)

    for b in range(batches):
        settled(b, 4, (final - 1) % 2).wait_send()
        settled(b, 2, final % 2).wait_send()
        settled(b, 2, 2).wait_send()


def finish(sites, last_ref, sums_ref, out_ref, moments_ref, sem):
    probes = last_ref.shape[0]
    copies = [
        pltpu.make_async_copy(last_ref.at[p], out_ref.at[p], sem.at[p]) for p in range(probes)
    ]
    for copy in copies:
        copy.start()
    mean = sums_ref[...] * (1.0 / sites)
    lane = lax.broadcasted_iota(jnp.int32, mean.shape, 1)
    base = jnp.where(lax.rem(lane, 2) == 0, mean[:, 0:1], mean[:, 1:2])
    moments_ref[...] = (2.0 * mean - base)[:, : 2 * STEPS]
    for copy in copies:
        copy.wait()


def solution(mesh):
    counts = (mesh.shape["gx"], mesh.shape["gy"])

    def local(probes, disorder, spectrum_center, half_width):
        n_probes, rows_x, rows_y, rows_z = probes.shape
        disorder = pltpu.with_memory_space_constraint(disorder, pltpu.HBM)
        smem = pl.BlockSpec(memory_space=pltpu.SMEM)
        vmem = pl.BlockSpec(memory_space=pltpu.VMEM)
        hbm = pl.BlockSpec(memory_space=pltpu.HBM)
        last, sums = pl.pallas_call(
            functools.partial(kernel, counts),
            out_shape=(
                jax.ShapeDtypeStruct(probes.shape, jnp.float32),
                jax.ShapeDtypeStruct((n_probes, 128), jnp.float32),
            ),
            in_specs=[smem, smem, hbm, hbm],
            out_specs=(vmem, vmem),
            scratch_shapes=[
                pltpu.VMEM((STEPS, n_probes, rows_x + 2, rows_y, rows_z), jnp.float32),
                pltpu.VMEM((rows_x, rows_y, rows_z), jnp.float32),
                pltpu.VMEM((STEPS, 2, n_probes, rows_x, rows_z), jnp.float32),
                pltpu.VMEM((STEPS, 2, n_probes, rows_x, rows_z), jnp.float32),
                pltpu.VMEM((2 * STEPS, n_probes, 8, 128), jnp.float32),
                pltpu.VMEM((3, 8, n_probes, 128), jnp.float32),
                pltpu.SemaphoreType.DMA((n_probes + 1,)),
                pltpu.SemaphoreType.DMA((3, n_probes // BATCH)),
                pltpu.SemaphoreType.DMA((3, n_probes // BATCH)),
                pltpu.SemaphoreType.DMA((3,)),
                pltpu.SemaphoreType.DMA((3,)),
                pltpu.SemaphoreType.REGULAR((2,)),
            ],
            compiler_params=pltpu.CompilerParams(
                collective_id=0, has_side_effects=True, vmem_limit_bytes=VMEM_LIMIT
            ),
        )(spectrum_center, half_width, probes, disorder)
        sites = rows_x * counts[0] * rows_y * counts[1] * rows_z
        return pl.pallas_call(
            functools.partial(finish, sites),
            out_shape=(
                jax.ShapeDtypeStruct(probes.shape, jnp.float32),
                jax.ShapeDtypeStruct((n_probes, 2 * STEPS), jnp.float32),
            ),
            in_specs=[vmem, vmem],
            out_specs=(hbm, vmem),
            scratch_shapes=[pltpu.SemaphoreType.DMA((n_probes,))],
            compiler_params=pltpu.CompilerParams(vmem_limit_bytes=8 * 1024 * 1024),
        )(last, sums)

    return jax.shard_map(
        local,
        mesh=mesh,
        in_specs=(P(None, "gx", "gy", None), P("gx", "gy", None), P(), P()),
        out_specs=(P(None, "gx", "gy", None), P()),
        check_vma=False,
    )
```

```python
import functools

import jax
import jax.numpy as jnp
from jax import lax
from jax.experimental import pallas as pl
from jax.experimental.pallas import tpu as pltpu
from jax.sharding import PartitionSpec as P

STEPS = 4
BATCH = 1
MESH = pl.DeviceIdType.MESH
LEAD = (5, 2)
ORDER = (0, 1, 2, 3)
UNROLL = 8
LATER = ((8, 8), (8, 8))
FINISH = (4, 8)
VMEM_LIMIT = 48 * 1024 * 1024


def kernel(
    counts, center_ref, width_ref, probes_ref, disorder_ref, last_ref, sums_ref,
    field, energy, rim_y, edge_y, parts, slots, load_sem, send_sem, recv_sem,
    slot_send, slot_recv, ready
):
    probes, rows_x, rows_y, rows_z = probes_ref.shape
    batches = probes // BATCH
    n_gx, n_gy = counts
    gx, gy = lax.axis_index("gx"), lax.axis_index("gy")
    beside = (
        (lax.rem(gx + 1, n_gx), gy),
        (lax.rem(gx + n_gx - 1, n_gx), gy),
        (gx, lax.rem(gy + 1, n_gy)),
        (gx, lax.rem(gy + n_gy - 1, n_gy)),
    )
    x_lo, x_hi, core = lax.rem(gx, 2), lax.rem(gy // 2, 2), lax.rem(gy, 2)
    chip_x, chip_y, chip_z = 2 * x_hi + x_lo, gy // 4, gx // 2
    wide_y, wide_z = n_gy // 4, n_gx // 2

    def device(x, y, z, c):
        return (2 * z + lax.rem(x, 2), 4 * y + 2 * (x // 2) + c)

    def group(pairs):
        return [device(lax.rem(chip_x + x, 4), lax.rem(chip_y + y, wide_y), lax.rem(chip_z + z, wide_z),
                       lax.rem(core + c, 2)) for x, y, z, c in pairs]

    group_x = group([(x, 0, 0, c) for x in range(4) for c in range(2) if x or c])
    group_yz = group([(0, y, z, 0) for y in range(wide_y) for z in range(wide_z) if y or z])
    groups = ((group_yz, chip_y * wide_z + chip_z), (group_x, 2 * chip_x + core))

    partner = (gx + 1 - 2 * x_lo, gy)
    across = (lax.rem(gx + 2 * x_lo + n_gx - 1, n_gx), gy)
    pairs = list(beside[2:]) + group_yz + group([(2, 0, 0, 0), (0, 0, 0, 1), (2, 0, 0, 1)])
    barrier = pltpu.get_barrier_semaphore()

    def tell(semaphore, peer):
        pl.semaphore_signal(
            semaphore, inc=1, device_id={"gx": peer[0], "gy": peer[1]}, device_id_type=MESH
        )

    @pl.when(x_lo == 1)
    def _():
        tell(barrier, partner)

    for x, y in pairs:
        tell(barrier, (x + 1 - lax.rem(x, 2), y))

    def load(p):
        return pltpu.make_async_copy(
            probes_ref.at[p], field.at[0, p, pl.ds(1, rows_x)], load_sem.at[p]
        )

    def load_energy():
        return pltpu.make_async_copy(disorder_ref, energy, load_sem.at[probes])

    def begin(p, carry):
        load(p).start()
        return carry

    lax.fori_loop(0, probes, begin, 0)
    load_energy().start()

    def faces(n, b):
        group = pl.ds(b * BATCH, BATCH)
        return (
            (field.at[n, group, rows_x], field.at[n, group, 0]),
            (field.at[n, group, 1], field.at[n, group, rows_x + 1]),
            (edge_y.at[n, 1, group], rim_y.at[n, 0, group]),
            (edge_y.at[n, 0, group], rim_y.at[n, 1, group]),
        )

    def start(src, dst, peer, sem, b):
        pltpu.make_async_remote_copy(
            src_ref=src,
            dst_ref=dst,
            send_sem=send_sem.at[sem, b],
            recv_sem=recv_sem.at[sem, b],
            device_id={"gx": peer[0], "gy": peer[1]},
            device_id_type=MESH,
        ).start()

    def send(n, b, which, sem):
        for f in which:
            src, dst = faces(n, b)[f]
            start(src, dst, beside[f], sem, b)

    def settled(b, count, sem):
        whole = field.at[0, 0, pl.ds(0, count * BATCH)]
        return pltpu.make_async_remote_copy(
            src_ref=whole,
            dst_ref=whole,
            send_sem=send_sem.at[sem, b],
            recv_sem=recv_sem.at[sem, b],
            device_id={"gx": beside[0][0], "gy": beside[0][1]},
            device_id_type=MESH,
        )

    @pl.when(x_lo == 0)
    def _():
        pl.semaphore_wait(barrier, 1)
        tell(ready.at[0], partner)

    @pl.when(x_lo == 1)
    def _():
        pl.semaphore_wait(ready.at[0], 1)

    def pair_first(b, carry):
        for q in range(BATCH):
            load(b * BATCH + q).wait()
        which = pl.ds(b * BATCH, BATCH)
        start(
            field.at[0, which, rows_x - (rows_x - 1) * x_lo],
            field.at[0, which, (rows_x + 1) * x_lo],
            partner, 0, b,
        )
        return carry

    lax.fori_loop(0, batches, pair_first, 0)

    def pack(p, carry):
        for x in range(rows_x):
            edge_y[0, 0, p, x : x + 1, :] = field[0, p, x + 1, 0:1, :]
            edge_y[0, 1, p, x : x + 1, :] = field[0, p, x + 1, rows_y - 1 : rows_y, :]
        return carry

    lax.fori_loop(0, probes, pack, 0)

    @pl.when(x_lo == 1)
    def _():
        pl.semaphore_wait(barrier, 2 * len(pairs))
        tell(ready.at[1], partner)

    @pl.when(x_lo == 0)
    def _():
        pl.semaphore_wait(ready.at[1], 1)

    def others(b, carry):
        which = pl.ds(b * BATCH, BATCH)
        start(
            field.at[0, which, 1 + (rows_x - 1) * x_lo],
            field.at[0, which, (rows_x + 1) * (1 - x_lo)],
            across, 0, b,
        )
        send(0, b, (2, 3), 0)
        return carry

    lax.fori_loop(0, batches, others, 0)
    load_energy().wait()
    energy[...] = energy[...] - center_ref[0]

    row = lax.broadcasted_iota(jnp.int32, (rows_y, rows_z), 0)
    scale = 1.0 / width_ref[0]
    zero = jnp.zeros((8, 128), jnp.float32)

    def fold(product):
        total = product[0:8]
        for start in range(8, rows_y, 8):
            total = total + product[start : start + 8]
        out = total[:, 0:128]
        for start in range(128, rows_z, 128):
            out = out + total[:, start : start + 128]
        return out

    def low_side(n, p, x, middle):
        y = jnp.where(row == 0, rim_y[n, 0, p, pl.ds(x, 1), :], pltpu.roll(middle, 1, 0))
        return field[n, p, x] + y + pltpu.roll(middle, 1, 1)

    def high_side(n, p, x, middle):
        y = jnp.where(
            row == rows_y - 1, rim_y[n, 1, p, pl.ds(x, 1), :], pltpu.roll(middle, rows_y - 1, 0)
        )
        return field[n, p, x + 2] + y + pltpu.roll(middle, rows_z - 1, 1)

    def advance(n, p):
        def plane(x, acc):
            square, cross = acc
            middle = field[n, p, x + 1]
            total = low_side(n, p, x, middle) + high_side(n, p, x, middle)
            new = (energy[x] * middle - total) * (scale if n == 0 else 2.0 * scale)
            if n > 0:
                new = new - field[n - 1, p, x + 1]
            field[n + 1, p, x + 1] = new
            edge_y[n + 1, 0, p, pl.ds(x, 1), :] = new[0:1]
            edge_y[n + 1, 1, p, pl.ds(x, 1), :] = new[rows_y - 1 : rows_y]
            return square + fold(middle * middle), cross + fold(new * middle)

        parts[2 * n, p], parts[2 * n + 1, p] = lax.fori_loop(0, rows_x, plane, (zero, zero), unroll=UNROLL)

    final = STEPS - 1

    def last_low(p):
        def plane(x, acc):
            square, cross = acc
            middle = field[final, p, x + 1]
            low = (2.0 * scale) * low_side(final, p, x, middle)
            new = (2.0 * scale) * energy[x] * middle - low - field[final - 1, p, x + 1]
            last_ref[p, x] = new
            return square + fold(middle * middle), cross + fold((new - low) * middle)

        parts[2 * final, p], parts[2 * final + 1, p] = lax.fori_loop(0, rows_x, plane, (zero, zero), unroll=UNROLL)

    def last_high(p):
        def plane(x, carry):
            middle = field[final, p, x + 1]
            last_ref[p, x] = last_ref[p, x] - (2.0 * scale) * high_side(final, p, x, middle)
            return carry

        lax.fori_loop(0, rows_x, plane, 0, unroll=UNROLL)

    for n in range(final):

        def batch(b, carry):
            settled(b, 4, n % 2).wait_recv()

            def one(q, carry):
                advance(n, b * BATCH + q)
                return carry

            lax.fori_loop(0, BATCH, one, 0)
            if n > 0:
                settled(b, 4, (n + 1) % 2).wait_send()
            send(n + 1, b, ORDER if n + 1 < final else (0, 2), (n + 1) % 2)
            return carry

        lax.fori_loop(0, batches, batch, 0)

    sent, done = [max(batches - lead, 0) for lead in LEAD], [0]

    def send_more(of_core, count):
        low = sent[of_core]
        sent[of_core] = min(low + count, batches)
        if sent[of_core] > low:

            @pl.when(core == of_core)
            def _():
                def one(b, carry):
                    send(final, b, (1, 3), 2)
                    return carry

                lax.fori_loop(low, sent[of_core], one, 0)

    def finish_more(count):
        low = done[0]
        done[0] = max(low, min(low + count, *sent))

        def one(b, carry):
            settled(b, 2, 2).wait_recv()
            for q in range(BATCH):
                last_high(b * BATCH + q)
            return carry

        if done[0] > low:
            lax.fori_loop(low, done[0], one, 0)

    lane = lax.broadcasted_iota(jnp.int32, (probes, 128), 1)

    def column_sums(sums, columns):
        for j in columns:
            column = jnp.sum(jnp.sum(parts[j], axis=1), axis=1, keepdims=True)
            sums = jnp.where(lane == j, column, sums)
        return sums

    sums = column_sums(jnp.zeros((probes, 128), jnp.float32), range(2 * final))

    def low_half(b, carry):
        settled(b, 2, final % 2).wait_recv()
        for q in range(BATCH):
            last_low(b * BATCH + q)
        if LEAD[0] == LEAD[1]:

            @pl.when(b >= LEAD[0])
            def _():
                send(final, b - LEAD[0], (1, 3), 2)
        else:

            @pl.when((b >= LEAD[0]) & (core == 0))
            def _():
                send(final, b - LEAD[0], (1, 3), 2)

            @pl.when((b >= LEAD[1]) & (core == 1))
            def _():
                send(final, b - LEAD[1], (1, 3), 2)

        return carry

    lax.fori_loop(0, batches, low_half, 0)
    sums = column_sums(sums, range(2 * final, 2 * STEPS))

    for g, (peers, place) in enumerate(groups):
        slots[g, place] = sums
        for x, y in peers:
            pltpu.make_async_remote_copy(
                src_ref=slots.at[g, place],
                dst_ref=slots.at[g, place],
                send_sem=slot_send.at[g],
                recv_sem=slot_recv.at[g],
                device_id={"gx": x, "gy": y},
                device_id_type=MESH,
            ).start()
        for of_core in range(2):
            send_more(of_core, LATER[of_core][g])
        finish_more(FINISH[g])
        whole = slots.at[g, pl.ds(0, len(peers))]
        arrived = pltpu.make_async_remote_copy(
            src_ref=whole,
            dst_ref=whole,
            send_sem=slot_send.at[g],
            recv_sem=slot_recv.at[g],
            device_id={"gx": peers[0][0], "gy": peers[0][1]},
            device_id_type=MESH,
        )
        arrived.wait_recv()
        sums = slots[g, 0]
        for i in range(1, len(peers) + 1):
            sums = sums + slots[g, i]
        arrived.wait_send()
    sums_ref[...] = sums
    finish_more(batches)

    def drain(b, carry):
        settled(b, 4, (final - 1) % 2).wait_send()
        settled(b, 2, final % 2).wait_send()
        settled(b, 2, 2).wait_send()
        return carry

    lax.fori_loop(0, batches, drain, 0)


def finish(sites, last_ref, sums_ref, out_ref, moments_ref, sem):
    probes = last_ref.shape[0]
    copies = [
        pltpu.make_async_copy(last_ref.at[p], out_ref.at[p], sem.at[p]) for p in range(probes)
    ]
    for copy in copies:
        copy.start()
    mean = sums_ref[...] * (1.0 / sites)
    lane = lax.broadcasted_iota(jnp.int32, mean.shape, 1)
    base = jnp.where(lax.rem(lane, 2) == 0, mean[:, 0:1], mean[:, 1:2])
    moments_ref[...] = (2.0 * mean - base)[:, : 2 * STEPS]
    for copy in copies:
        copy.wait()


def solution(mesh):
    counts = (mesh.shape["gx"], mesh.shape["gy"])

    def local(probes, disorder, spectrum_center, half_width):
        n_probes, rows_x, rows_y, rows_z = probes.shape
        disorder = pltpu.with_memory_space_constraint(disorder, pltpu.HBM)
        smem = pl.BlockSpec(memory_space=pltpu.SMEM)
        vmem = pl.BlockSpec(memory_space=pltpu.VMEM)
        hbm = pl.BlockSpec(memory_space=pltpu.HBM)
        last, sums = pl.pallas_call(
            functools.partial(kernel, counts),
            out_shape=(
                jax.ShapeDtypeStruct(probes.shape, jnp.float32),
                jax.ShapeDtypeStruct((n_probes, 128), jnp.float32),
            ),
            in_specs=[smem, smem, hbm, hbm],
            out_specs=(vmem, vmem),
            scratch_shapes=[
                pltpu.VMEM((STEPS, n_probes, rows_x + 2, rows_y, rows_z), jnp.float32),
                pltpu.VMEM((rows_x, rows_y, rows_z), jnp.float32),
                pltpu.VMEM((STEPS, 2, n_probes, rows_x, rows_z), jnp.float32),
                pltpu.VMEM((STEPS, 2, n_probes, rows_x, rows_z), jnp.float32),
                pltpu.VMEM((2 * STEPS, n_probes, 8, 128), jnp.float32),
                pltpu.VMEM((2, 16, n_probes, 128), jnp.float32),
                pltpu.SemaphoreType.DMA((n_probes + 1,)),
                pltpu.SemaphoreType.DMA((3, n_probes // BATCH)),
                pltpu.SemaphoreType.DMA((3, n_probes // BATCH)),
                pltpu.SemaphoreType.DMA((3,)),
                pltpu.SemaphoreType.DMA((3,)),
                pltpu.SemaphoreType.REGULAR((2,)),
            ],
            compiler_params=pltpu.CompilerParams(
                collective_id=0, has_side_effects=True, vmem_limit_bytes=VMEM_LIMIT
            ),
        )(spectrum_center, half_width, probes, disorder)
        sites = rows_x * counts[0] * rows_y * counts[1] * rows_z
        return pl.pallas_call(
            functools.partial(finish, sites),
            out_shape=(
                jax.ShapeDtypeStruct(probes.shape, jnp.float32),
                jax.ShapeDtypeStruct((n_probes, 2 * STEPS), jnp.float32),
            ),
            in_specs=[vmem, vmem],
            out_specs=(hbm, vmem),
            scratch_shapes=[pltpu.SemaphoreType.DMA((n_probes,))],
            compiler_params=pltpu.CompilerParams(vmem_limit_bytes=8 * 1024 * 1024),
        )(last, sums)

    return jax.shard_map(
        local,
        mesh=mesh,
        in_specs=(P(None, "gx", "gy", None), P("gx", "gy", None), P(), P()),
        out_specs=(P(None, "gx", "gy", None), P()),
        check_vma=False,
    )
```

```python
import functools

import jax
import jax.numpy as jnp
from jax import lax
from jax.experimental import pallas as pl
from jax.experimental.pallas import tpu as pltpu
from jax.sharding import PartitionSpec as P

STEPS = 4
BATCH = 1
MESH = pl.DeviceIdType.MESH
LEAD = (5, 2)
ORDER = (3, 2, 1, 0)
UNROLL = 16
LATER = ((8, 8), (8, 8))
FINISH = (4, 8)
VMEM_LIMIT = 48 * 1024 * 1024


def kernel(
    counts, center_ref, width_ref, probes_ref, disorder_ref, last_ref, sums_ref,
    field, energy, rim_y, edge_y, parts, slots, load_sem, send_sem, recv_sem,
    slot_send, slot_recv, ready
):
    probes, rows_x, rows_y, rows_z = probes_ref.shape
    batches = probes // BATCH
    n_gx, n_gy = counts
    gx, gy = lax.axis_index("gx"), lax.axis_index("gy")
    beside = (
        (lax.rem(gx + 1, n_gx), gy),
        (lax.rem(gx + n_gx - 1, n_gx), gy),
        (gx, lax.rem(gy + 1, n_gy)),
        (gx, lax.rem(gy + n_gy - 1, n_gy)),
    )
    x_lo, x_hi, core = lax.rem(gx, 2), lax.rem(gy // 2, 2), lax.rem(gy, 2)
    chip_x, chip_y, chip_z = 2 * x_hi + x_lo, gy // 4, gx // 2
    wide_y, wide_z = n_gy // 4, n_gx // 2

    def device(x, y, z, c):
        return (2 * z + lax.rem(x, 2), 4 * y + 2 * (x // 2) + c)

    def group(pairs):
        return [device(lax.rem(chip_x + x, 4), lax.rem(chip_y + y, wide_y), lax.rem(chip_z + z, wide_z),
                       lax.rem(core + c, 2)) for x, y, z, c in pairs]

    group_x = group([(x, 0, 0, c) for x in range(4) for c in range(2) if x or c])
    group_yz = group([(0, y, z, 0) for y in range(wide_y) for z in range(wide_z) if y or z])
    groups = ((group_yz, chip_y * wide_z + chip_z), (group_x, 2 * chip_x + core))

    partner = (gx + 1 - 2 * x_lo, gy)
    across = (lax.rem(gx + 2 * x_lo + n_gx - 1, n_gx), gy)
    pairs = list(beside[2:]) + group_yz + group([(2, 0, 0, 0), (0, 0, 0, 1), (2, 0, 0, 1)])
    barrier = pltpu.get_barrier_semaphore()

    def tell(semaphore, peer):
        pl.semaphore_signal(
            semaphore, inc=1, device_id={"gx": peer[0], "gy": peer[1]}, device_id_type=MESH
        )

    @pl.when(x_lo == 1)
    def _():
        tell(barrier, partner)

    for x, y in pairs:
        tell(barrier, (x + 1 - lax.rem(x, 2), y))

    def load(p):
        return pltpu.make_async_copy(
            probes_ref.at[p], field.at[0, p, pl.ds(1, rows_x)], load_sem.at[p]
        )

    def load_energy():
        return pltpu.make_async_copy(disorder_ref, energy, load_sem.at[probes])

    def begin(p, carry):
        load(p).start()
        return carry

    lax.fori_loop(0, probes, begin, 0)
    load_energy().start()

    def faces(n, b):
        group = pl.ds(b * BATCH, BATCH)
        return (
            (field.at[n, group, rows_x], field.at[n, group, 0]),
            (field.at[n, group, 1], field.at[n, group, rows_x + 1]),
            (edge_y.at[n, 1, group], rim_y.at[n, 0, group]),
            (edge_y.at[n, 0, group], rim_y.at[n, 1, group]),
        )

    def start(src, dst, peer, sem, b):
        pltpu.make_async_remote_copy(
            src_ref=src,
            dst_ref=dst,
            send_sem=send_sem.at[sem, b],
            recv_sem=recv_sem.at[sem, b],
            device_id={"gx": peer[0], "gy": peer[1]},
            device_id_type=MESH,
        ).start()

    def send(n, b, which, sem):
        for f in which:
            src, dst = faces(n, b)[f]
            start(src, dst, beside[f], sem, b)

    def settled(b, count, sem):
        whole = field.at[0, 0, pl.ds(0, count * BATCH)]
        return pltpu.make_async_remote_copy(
            src_ref=whole,
            dst_ref=whole,
            send_sem=send_sem.at[sem, b],
            recv_sem=recv_sem.at[sem, b],
            device_id={"gx": beside[0][0], "gy": beside[0][1]},
            device_id_type=MESH,
        )

    @pl.when(x_lo == 0)
    def _():
        pl.semaphore_wait(barrier, 1)
        tell(ready.at[0], partner)

    @pl.when(x_lo == 1)
    def _():
        pl.semaphore_wait(ready.at[0], 1)

    def pair_first(b, carry):
        for q in range(BATCH):
            load(b * BATCH + q).wait()
        which = pl.ds(b * BATCH, BATCH)
        start(
            field.at[0, which, rows_x - (rows_x - 1) * x_lo],
            field.at[0, which, (rows_x + 1) * x_lo],
            partner, 0, b,
        )
        return carry

    lax.fori_loop(0, batches, pair_first, 0)

    def pack(p, carry):
        for x in range(rows_x):
            edge_y[0, 0, p, x : x + 1, :] = field[0, p, x + 1, 0:1, :]
            edge_y[0, 1, p, x : x + 1, :] = field[0, p, x + 1, rows_y - 1 : rows_y, :]
        return carry

    lax.fori_loop(0, probes, pack, 0)

    @pl.when(x_lo == 1)
    def _():
        pl.semaphore_wait(barrier, 2 * len(pairs))
        tell(ready.at[1], partner)

    @pl.when(x_lo == 0)
    def _():
        pl.semaphore_wait(ready.at[1], 1)

    def others(b, carry):
        which = pl.ds(b * BATCH, BATCH)
        start(
            field.at[0, which, 1 + (rows_x - 1) * x_lo],
            field.at[0, which, (rows_x + 1) * (1 - x_lo)],
            across, 0, b,
        )
        send(0, b, (2, 3), 0)
        return carry

    lax.fori_loop(0, batches, others, 0)
    load_energy().wait()
    energy[...] = energy[...] - center_ref[0]

    row = lax.broadcasted_iota(jnp.int32, (rows_y, rows_z), 0)
    scale = 1.0 / width_ref[0]
    zero = jnp.zeros((8, 128), jnp.float32)

    def fold(product):
        total = product[0:8]
        for start in range(8, rows_y, 8):
            total = total + product[start : start + 8]
        out = total[:, 0:128]
        for start in range(128, rows_z, 128):
            out = out + total[:, start : start + 128]
        return out

    def low_side(n, p, x, middle):
        y = jnp.where(row == 0, rim_y[n, 0, p, pl.ds(x, 1), :], pltpu.roll(middle, 1, 0))
        return field[n, p, x] + y + pltpu.roll(middle, 1, 1)

    def high_side(n, p, x, middle):
        y = jnp.where(
            row == rows_y - 1, rim_y[n, 1, p, pl.ds(x, 1), :], pltpu.roll(middle, rows_y - 1, 0)
        )
        return field[n, p, x + 2] + y + pltpu.roll(middle, rows_z - 1, 1)

    def advance(n, p):
        def plane(x, acc):
            square, cross = acc
            middle = field[n, p, x + 1]
            total = low_side(n, p, x, middle) + high_side(n, p, x, middle)
            new = (energy[x] * middle - total) * (scale if n == 0 else 2.0 * scale)
            if n > 0:
                new = new - field[n - 1, p, x + 1]
            field[n + 1, p, x + 1] = new
            edge_y[n + 1, 0, p, pl.ds(x, 1), :] = new[0:1]
            edge_y[n + 1, 1, p, pl.ds(x, 1), :] = new[rows_y - 1 : rows_y]
            return square + fold(middle * middle), cross + fold(new * middle)

        parts[2 * n, p], parts[2 * n + 1, p] = lax.fori_loop(0, rows_x, plane, (zero, zero), unroll=UNROLL)

    final = STEPS - 1

    def last_low(p):
        def plane(x, acc):
            square, cross = acc
            middle = field[final, p, x + 1]
            low = (2.0 * scale) * low_side(final, p, x, middle)
            new = (2.0 * scale) * energy[x] * middle - low - field[final - 1, p, x + 1]
            last_ref[p, x] = new
            return square + fold(middle * middle), cross + fold((new - low) * middle)

        parts[2 * final, p], parts[2 * final + 1, p] = lax.fori_loop(0, rows_x, plane, (zero, zero), unroll=UNROLL)

    def last_high(p):
        def plane(x, carry):
            middle = field[final, p, x + 1]
            last_ref[p, x] = last_ref[p, x] - (2.0 * scale) * high_side(final, p, x, middle)
            return carry

        lax.fori_loop(0, rows_x, plane, 0, unroll=UNROLL)

    for n in range(final):

        def batch(b, carry):
            settled(b, 4, n % 2).wait_recv()

            def one(q, carry):
                advance(n, b * BATCH + q)
                return carry

            lax.fori_loop(0, BATCH, one, 0)
            if n > 0:
                settled(b, 4, (n + 1) % 2).wait_send()
            send(n + 1, b, ORDER if n + 1 < final else (2, 0), (n + 1) % 2)
            return carry

        lax.fori_loop(0, batches, batch, 0)

    sent, done = [max(batches - lead, 0) for lead in LEAD], [0]

    def send_more(of_core, count):
        low = sent[of_core]
        sent[of_core] = min(low + count, batches)
        if sent[of_core] > low:

            @pl.when(core == of_core)
            def _():
                def one(b, carry):
                    send(final, b, (3, 1), 2)
                    return carry

                lax.fori_loop(low, sent[of_core], one, 0)

    def finish_more(count):
        low = done[0]
        done[0] = max(low, min(low + count, *sent))

        def one(b, carry):
            settled(b, 2, 2).wait_recv()
            for q in range(BATCH):
                last_high(b * BATCH + q)
            return carry

        if done[0] > low:
            lax.fori_loop(low, done[0], one, 0)

    lane = lax.broadcasted_iota(jnp.int32, (probes, 128), 1)

    def column_sums(sums, columns):
        for j in columns:
            column = jnp.sum(jnp.sum(parts[j], axis=1), axis=1, keepdims=True)
            sums = jnp.where(lane == j, column, sums)
        return sums

    sums = column_sums(jnp.zeros((probes, 128), jnp.float32), range(2 * final))

    def low_half(b, carry):
        settled(b, 2, final % 2).wait_recv()
        for q in range(BATCH):
            last_low(b * BATCH + q)
        if LEAD[0] == LEAD[1]:

            @pl.when(b >= LEAD[0])
            def _():
                send(final, b - LEAD[0], (3, 1), 2)
        else:

            @pl.when((b >= LEAD[0]) & (core == 0))
            def _():
                send(final, b - LEAD[0], (3, 1), 2)

            @pl.when((b >= LEAD[1]) & (core == 1))
            def _():
                send(final, b - LEAD[1], (3, 1), 2)

        return carry

    lax.fori_loop(0, batches, low_half, 0)
    sums = column_sums(sums, range(2 * final, 2 * STEPS))

    for g, (peers, place) in enumerate(groups):
        slots[g, place] = sums
        for x, y in peers:
            pltpu.make_async_remote_copy(
                src_ref=slots.at[g, place],
                dst_ref=slots.at[g, place],
                send_sem=slot_send.at[g],
                recv_sem=slot_recv.at[g],
                device_id={"gx": x, "gy": y},
                device_id_type=MESH,
            ).start()
        for of_core in range(2):
            send_more(of_core, LATER[of_core][g])
        finish_more(FINISH[g])
        whole = slots.at[g, pl.ds(0, len(peers))]
        arrived = pltpu.make_async_remote_copy(
            src_ref=whole,
            dst_ref=whole,
            send_sem=slot_send.at[g],
            recv_sem=slot_recv.at[g],
            device_id={"gx": peers[0][0], "gy": peers[0][1]},
            device_id_type=MESH,
        )
        arrived.wait_recv()
        sums = slots[g, 0]
        for i in range(1, len(peers) + 1):
            sums = sums + slots[g, i]
        arrived.wait_send()
    sums_ref[...] = sums
    finish_more(batches)

    def drain(b, carry):
        settled(b, 4, (final - 1) % 2).wait_send()
        settled(b, 2, final % 2).wait_send()
        settled(b, 2, 2).wait_send()
        return carry

    lax.fori_loop(0, batches, drain, 0)


def finish(sites, last_ref, sums_ref, out_ref, moments_ref, sem):
    probes = last_ref.shape[0]
    copies = [
        pltpu.make_async_copy(last_ref.at[p], out_ref.at[p], sem.at[p]) for p in range(probes)
    ]
    for copy in copies:
        copy.start()
    mean = sums_ref[...] * (1.0 / sites)
    lane = lax.broadcasted_iota(jnp.int32, mean.shape, 1)
    base = jnp.where(lax.rem(lane, 2) == 0, mean[:, 0:1], mean[:, 1:2])
    moments_ref[...] = (2.0 * mean - base)[:, : 2 * STEPS]
    for copy in copies:
        copy.wait()


def solution(mesh):
    counts = (mesh.shape["gx"], mesh.shape["gy"])

    def local(probes, disorder, spectrum_center, half_width):
        n_probes, rows_x, rows_y, rows_z = probes.shape
        disorder = pltpu.with_memory_space_constraint(disorder, pltpu.HBM)
        smem = pl.BlockSpec(memory_space=pltpu.SMEM)
        vmem = pl.BlockSpec(memory_space=pltpu.VMEM)
        hbm = pl.BlockSpec(memory_space=pltpu.HBM)
        last, sums = pl.pallas_call(
            functools.partial(kernel, counts),
            out_shape=(
                jax.ShapeDtypeStruct(probes.shape, jnp.float32),
                jax.ShapeDtypeStruct((n_probes, 128), jnp.float32),
            ),
            in_specs=[smem, smem, hbm, hbm],
            out_specs=(vmem, vmem),
            scratch_shapes=[
                pltpu.VMEM((STEPS, n_probes, rows_x + 2, rows_y, rows_z), jnp.float32),
                pltpu.VMEM((rows_x, rows_y, rows_z), jnp.float32),
                pltpu.VMEM((STEPS, 2, n_probes, rows_x, rows_z), jnp.float32),
                pltpu.VMEM((STEPS, 2, n_probes, rows_x, rows_z), jnp.float32),
                pltpu.VMEM((2 * STEPS, n_probes, 8, 128), jnp.float32),
                pltpu.VMEM((2, 16, n_probes, 128), jnp.float32),
                pltpu.SemaphoreType.DMA((n_probes + 1,)),
                pltpu.SemaphoreType.DMA((3, n_probes // BATCH)),
                pltpu.SemaphoreType.DMA((3, n_probes // BATCH)),
                pltpu.SemaphoreType.DMA((3,)),
                pltpu.SemaphoreType.DMA((3,)),
                pltpu.SemaphoreType.REGULAR((2,)),
            ],
            compiler_params=pltpu.CompilerParams(
                collective_id=0, has_side_effects=True, vmem_limit_bytes=VMEM_LIMIT
            ),
        )(spectrum_center, half_width, probes, disorder)
        sites = rows_x * counts[0] * rows_y * counts[1] * rows_z
        return pl.pallas_call(
            functools.partial(finish, sites),
            out_shape=(
                jax.ShapeDtypeStruct(probes.shape, jnp.float32),
                jax.ShapeDtypeStruct((n_probes, 2 * STEPS), jnp.float32),
            ),
            in_specs=[vmem, vmem],
            out_specs=(hbm, vmem),
            scratch_shapes=[pltpu.SemaphoreType.DMA((n_probes,))],
            compiler_params=pltpu.CompilerParams(vmem_limit_bytes=8 * 1024 * 1024),
        )(last, sums)

    return jax.shard_map(
        local,
        mesh=mesh,
        in_specs=(P(None, "gx", "gy", None), P("gx", "gy", None), P(), P()),
        out_specs=(P(None, "gx", "gy", None), P()),
        check_vma=False,
    )
```

```python
import functools

import jax
import jax.numpy as jnp
from jax import lax
from jax.experimental import pallas as pl
from jax.experimental.pallas import tpu as pltpu
from jax.sharding import PartitionSpec as P

STEPS = 4
BATCH = 1
MESH = pl.DeviceIdType.MESH
LEAD = (5, 2)
ORDER = (3, 2, 1, 0)
UNROLL = 16
LATER = ((8, 8), (8, 8))
FINISH = (4, 8)
VMEM_LIMIT = 48 * 1024 * 1024


def kernel(
    counts, center_ref, width_ref, probes_ref, disorder_ref, last_ref, sums_ref,
    field, energy, rim_y, edge_y, parts, slots, load_sem, send_sem, recv_sem,
    slot_send, slot_recv, ready
):
    probes, rows_x, rows_y, rows_z = probes_ref.shape
    batches = probes // BATCH
    n_gx, n_gy = counts
    gx, gy = lax.axis_index("gx"), lax.axis_index("gy")
    beside = (
        (lax.rem(gx + 1, n_gx), gy),
        (lax.rem(gx + n_gx - 1, n_gx), gy),
        (gx, lax.rem(gy + 1, n_gy)),
        (gx, lax.rem(gy + n_gy - 1, n_gy)),
    )
    x_lo, x_hi, core = lax.rem(gx, 2), lax.rem(gy // 2, 2), lax.rem(gy, 2)
    chip_x, chip_y, chip_z = 2 * x_hi + x_lo, gy // 4, gx // 2
    wide_y, wide_z = n_gy // 4, n_gx // 2

    def device(x, y, z, c):
        return (2 * z + lax.rem(x, 2), 4 * y + 2 * (x // 2) + c)

    def hops(step):
        x, y, z, c = step
        return -(min(x, 4 - x) + min(y, wide_y - y) + min(z, wide_z - z))

    def group(pairs):
        return [device(lax.rem(chip_x + x, 4), lax.rem(chip_y + y, wide_y), lax.rem(chip_z + z, wide_z),
                       lax.rem(core + c, 2)) for x, y, z, c in sorted(pairs, key=hops)]

    group_x = group([(x, 0, 0, c) for x in range(4) for c in range(2) if x or c])
    group_yz = group([(0, y, z, 0) for y in range(wide_y) for z in range(wide_z) if y or z])
    groups = ((group_yz, chip_y * wide_z + chip_z), (group_x, 2 * chip_x + core))

    partner = (gx + 1 - 2 * x_lo, gy)
    across = (lax.rem(gx + 2 * x_lo + n_gx - 1, n_gx), gy)
    pairs = list(beside[2:]) + group_yz + group([(2, 0, 0, 0), (0, 0, 0, 1), (2, 0, 0, 1)])
    barrier = pltpu.get_barrier_semaphore()

    def tell(semaphore, peer):
        pl.semaphore_signal(
            semaphore, inc=1, device_id={"gx": peer[0], "gy": peer[1]}, device_id_type=MESH
        )

    @pl.when(x_lo == 1)
    def _():
        tell(barrier, partner)

    for x, y in pairs:
        tell(barrier, (x + 1 - lax.rem(x, 2), y))

    def load(p):
        return pltpu.make_async_copy(
            probes_ref.at[p], field.at[0, p, pl.ds(1, rows_x)], load_sem.at[p]
        )

    def load_energy():
        return pltpu.make_async_copy(disorder_ref, energy, load_sem.at[probes])

    def begin(p, carry):
        load(p).start()
        return carry

    lax.fori_loop(0, probes, begin, 0)
    load_energy().start()

    def faces(n, b):
        group = pl.ds(b * BATCH, BATCH)
        return (
            (field.at[n, group, rows_x], field.at[n, group, 0]),
            (field.at[n, group, 1], field.at[n, group, rows_x + 1]),
            (edge_y.at[n, 1, group], rim_y.at[n, 0, group]),
            (edge_y.at[n, 0, group], rim_y.at[n, 1, group]),
        )

    def start(src, dst, peer, sem, b):
        pltpu.make_async_remote_copy(
            src_ref=src,
            dst_ref=dst,
            send_sem=send_sem.at[sem, b],
            recv_sem=recv_sem.at[sem, b],
            device_id={"gx": peer[0], "gy": peer[1]},
            device_id_type=MESH,
        ).start()

    def send(n, b, which, sem):
        for f in which:
            src, dst = faces(n, b)[f]
            start(src, dst, beside[f], sem, b)

    def settled(b, count, sem):
        whole = field.at[0, 0, pl.ds(0, count * BATCH)]
        return pltpu.make_async_remote_copy(
            src_ref=whole,
            dst_ref=whole,
            send_sem=send_sem.at[sem, b],
            recv_sem=recv_sem.at[sem, b],
            device_id={"gx": beside[0][0], "gy": beside[0][1]},
            device_id_type=MESH,
        )

    @pl.when(x_lo == 0)
    def _():
        pl.semaphore_wait(barrier, 1)
        tell(ready.at[0], partner)

    @pl.when(x_lo == 1)
    def _():
        pl.semaphore_wait(ready.at[0], 1)

    def pair_first(b, carry):
        for q in range(BATCH):
            load(b * BATCH + q).wait()
        which = pl.ds(b * BATCH, BATCH)
        start(
            field.at[0, which, rows_x - (rows_x - 1) * x_lo],
            field.at[0, which, (rows_x + 1) * x_lo],
            partner, 0, b,
        )
        return carry

    lax.fori_loop(0, batches, pair_first, 0)

    def pack(p, carry):
        for x in range(rows_x):
            edge_y[0, 0, p, x : x + 1, :] = field[0, p, x + 1, 0:1, :]
            edge_y[0, 1, p, x : x + 1, :] = field[0, p, x + 1, rows_y - 1 : rows_y, :]
        return carry

    lax.fori_loop(0, probes, pack, 0)

    @pl.when(x_lo == 1)
    def _():
        pl.semaphore_wait(barrier, 2 * len(pairs))
        tell(ready.at[1], partner)

    @pl.when(x_lo == 0)
    def _():
        pl.semaphore_wait(ready.at[1], 1)

    def others(b, carry):
        which = pl.ds(b * BATCH, BATCH)
        start(
            field.at[0, which, 1 + (rows_x - 1) * x_lo],
            field.at[0, which, (rows_x + 1) * (1 - x_lo)],
            across, 0, b,
        )
        send(0, b, (2, 3), 0)
        return carry

    lax.fori_loop(0, batches, others, 0)
    load_energy().wait()
    energy[...] = energy[...] - center_ref[0]

    row = lax.broadcasted_iota(jnp.int32, (rows_y, rows_z), 0)
    scale = 1.0 / width_ref[0]
    zero = jnp.zeros((8, 128), jnp.float32)

    def fold(product):
        total = product[0:8]
        for start in range(8, rows_y, 8):
            total = total + product[start : start + 8]
        out = total[:, 0:128]
        for start in range(128, rows_z, 128):
            out = out + total[:, start : start + 128]
        return out

    def low_side(n, p, x, middle):
        y = jnp.where(row == 0, rim_y[n, 0, p, pl.ds(x, 1), :], pltpu.roll(middle, 1, 0))
        return field[n, p, x] + y + pltpu.roll(middle, 1, 1)

    def high_side(n, p, x, middle):
        y = jnp.where(
            row == rows_y - 1, rim_y[n, 1, p, pl.ds(x, 1), :], pltpu.roll(middle, rows_y - 1, 0)
        )
        return field[n, p, x + 2] + y + pltpu.roll(middle, rows_z - 1, 1)

    def advance(n, p):
        def plane(x, acc):
            square, cross = acc
            middle = field[n, p, x + 1]
            total = low_side(n, p, x, middle) + high_side(n, p, x, middle)
            new = (energy[x] * middle - total) * (scale if n == 0 else 2.0 * scale)
            if n > 0:
                new = new - field[n - 1, p, x + 1]
            field[n + 1, p, x + 1] = new
            edge_y[n + 1, 0, p, pl.ds(x, 1), :] = new[0:1]
            edge_y[n + 1, 1, p, pl.ds(x, 1), :] = new[rows_y - 1 : rows_y]
            return square + fold(middle * middle), cross + fold(new * middle)

        parts[2 * n, p], parts[2 * n + 1, p] = lax.fori_loop(0, rows_x, plane, (zero, zero), unroll=UNROLL)

    final = STEPS - 1

    def last_low(p):
        def plane(x, acc):
            square, cross = acc
            middle = field[final, p, x + 1]
            low = (2.0 * scale) * low_side(final, p, x, middle)
            new = (2.0 * scale) * energy[x] * middle - low - field[final - 1, p, x + 1]
            last_ref[p, x] = new
            return square + fold(middle * middle), cross + fold((new - low) * middle)

        parts[2 * final, p], parts[2 * final + 1, p] = lax.fori_loop(0, rows_x, plane, (zero, zero), unroll=UNROLL)

    def last_high(p):
        def plane(x, carry):
            middle = field[final, p, x + 1]
            last_ref[p, x] = last_ref[p, x] - (2.0 * scale) * high_side(final, p, x, middle)
            return carry

        lax.fori_loop(0, rows_x, plane, 0, unroll=UNROLL)

    for n in range(final):

        def batch(b, carry):
            settled(b, 4, n % 2).wait_recv()

            def one(q, carry):
                advance(n, b * BATCH + q)
                return carry

            lax.fori_loop(0, BATCH, one, 0)
            if n > 0:
                settled(b, 4, (n + 1) % 2).wait_send()
            send(n + 1, b, ORDER if n + 1 < final else (2, 0), (n + 1) % 2)
            return carry

        lax.fori_loop(0, batches, batch, 0)

    sent, done = [max(batches - lead, 0) for lead in LEAD], [0]

    def send_more(of_core, count):
        low = sent[of_core]
        sent[of_core] = min(low + count, batches)
        if sent[of_core] > low:

            @pl.when(core == of_core)
            def _():
                def one(b, carry):
                    send(final, b, (3, 1), 2)
                    return carry

                lax.fori_loop(low, sent[of_core], one, 0)

    def finish_more(count):
        low = done[0]
        done[0] = max(low, min(low + count, *sent))

        def one(b, carry):
            settled(b, 2, 2).wait_recv()
            for q in range(BATCH):
                last_high(b * BATCH + q)
            return carry

        if done[0] > low:
            lax.fori_loop(low, done[0], one, 0)

    lane = lax.broadcasted_iota(jnp.int32, (probes, 128), 1)

    def column_sums(sums, columns):
        for j in columns:
            column = jnp.sum(jnp.sum(parts[j], axis=1), axis=1, keepdims=True)
            sums = jnp.where(lane == j, column, sums)
        return sums

    sums = column_sums(jnp.zeros((probes, 128), jnp.float32), range(2 * final))

    def low_half(b, carry):
        settled(b, 2, final % 2).wait_recv()
        for q in range(BATCH):
            last_low(b * BATCH + q)
        if LEAD[0] == LEAD[1]:

            @pl.when(b >= LEAD[0])
            def _():
                send(final, b - LEAD[0], (3, 1), 2)
        else:

            @pl.when((b >= LEAD[0]) & (core == 0))
            def _():
                send(final, b - LEAD[0], (3, 1), 2)

            @pl.when((b >= LEAD[1]) & (core == 1))
            def _():
                send(final, b - LEAD[1], (3, 1), 2)

        return carry

    lax.fori_loop(0, batches, low_half, 0)
    sums = column_sums(sums, range(2 * final, 2 * STEPS))

    for g, (peers, place) in enumerate(groups):
        slots[g, place] = sums
        for x, y in peers:
            pltpu.make_async_remote_copy(
                src_ref=slots.at[g, place],
                dst_ref=slots.at[g, place],
                send_sem=slot_send.at[g],
                recv_sem=slot_recv.at[g],
                device_id={"gx": x, "gy": y},
                device_id_type=MESH,
            ).start()
        for of_core in range(2):
            send_more(of_core, LATER[of_core][g])
        finish_more(FINISH[g])
        whole = slots.at[g, pl.ds(0, len(peers))]
        arrived = pltpu.make_async_remote_copy(
            src_ref=whole,
            dst_ref=whole,
            send_sem=slot_send.at[g],
            recv_sem=slot_recv.at[g],
            device_id={"gx": peers[0][0], "gy": peers[0][1]},
            device_id_type=MESH,
        )
        arrived.wait_recv()
        sums = slots[g, 0]
        for i in range(1, len(peers) + 1):
            sums = sums + slots[g, i]
        arrived.wait_send()
    sums_ref[...] = sums
    finish_more(batches)

    def drain(b, carry):
        settled(b, 4, (final - 1) % 2).wait_send()
        settled(b, 2, final % 2).wait_send()
        settled(b, 2, 2).wait_send()
        return carry

    lax.fori_loop(0, batches, drain, 0)


def finish(sites, last_ref, sums_ref, out_ref, moments_ref, sem):
    probes = last_ref.shape[0]
    copies = [
        pltpu.make_async_copy(last_ref.at[p], out_ref.at[p], sem.at[p]) for p in range(probes)
    ]
    for copy in copies:
        copy.start()
    mean = sums_ref[...] * (1.0 / sites)
    lane = lax.broadcasted_iota(jnp.int32, mean.shape, 1)
    base = jnp.where(lax.rem(lane, 2) == 0, mean[:, 0:1], mean[:, 1:2])
    moments_ref[...] = (2.0 * mean - base)[:, : 2 * STEPS]
    for copy in copies:
        copy.wait()


def solution(mesh):
    counts = (mesh.shape["gx"], mesh.shape["gy"])

    def local(probes, disorder, spectrum_center, half_width):
        n_probes, rows_x, rows_y, rows_z = probes.shape
        disorder = pltpu.with_memory_space_constraint(disorder, pltpu.HBM)
        smem = pl.BlockSpec(memory_space=pltpu.SMEM)
        vmem = pl.BlockSpec(memory_space=pltpu.VMEM)
        hbm = pl.BlockSpec(memory_space=pltpu.HBM)
        last, sums = pl.pallas_call(
            functools.partial(kernel, counts),
            out_shape=(
                jax.ShapeDtypeStruct(probes.shape, jnp.float32),
                jax.ShapeDtypeStruct((n_probes, 128), jnp.float32),
            ),
            in_specs=[smem, smem, hbm, hbm],
            out_specs=(vmem, vmem),
            scratch_shapes=[
                pltpu.VMEM((STEPS, n_probes, rows_x + 2, rows_y, rows_z), jnp.float32),
                pltpu.VMEM((rows_x, rows_y, rows_z), jnp.float32),
                pltpu.VMEM((STEPS, 2, n_probes, rows_x, rows_z), jnp.float32),
                pltpu.VMEM((STEPS, 2, n_probes, rows_x, rows_z), jnp.float32),
                pltpu.VMEM((2 * STEPS, n_probes, 8, 128), jnp.float32),
                pltpu.VMEM((2, 16, n_probes, 128), jnp.float32),
                pltpu.SemaphoreType.DMA((n_probes + 1,)),
                pltpu.SemaphoreType.DMA((3, n_probes // BATCH)),
                pltpu.SemaphoreType.DMA((3, n_probes // BATCH)),
                pltpu.SemaphoreType.DMA((3,)),
                pltpu.SemaphoreType.DMA((3,)),
                pltpu.SemaphoreType.REGULAR((2,)),
            ],
            compiler_params=pltpu.CompilerParams(
                collective_id=0, has_side_effects=True, vmem_limit_bytes=VMEM_LIMIT
            ),
        )(spectrum_center, half_width, probes, disorder)
        sites = rows_x * counts[0] * rows_y * counts[1] * rows_z
        return pl.pallas_call(
            functools.partial(finish, sites),
            out_shape=(
                jax.ShapeDtypeStruct(probes.shape, jnp.float32),
                jax.ShapeDtypeStruct((n_probes, 2 * STEPS), jnp.float32),
            ),
            in_specs=[vmem, vmem],
            out_specs=(hbm, vmem),
            scratch_shapes=[pltpu.SemaphoreType.DMA((n_probes,))],
            compiler_params=pltpu.CompilerParams(vmem_limit_bytes=8 * 1024 * 1024),
        )(last, sums)

    return jax.shard_map(
        local,
        mesh=mesh,
        in_specs=(P(None, "gx", "gy", None), P("gx", "gy", None), P(), P()),
        out_specs=(P(None, "gx", "gy", None), P()),
        check_vma=False,
    )
```
